32 devices in a mesh: sec: 8 (over z, x), chan: 4 (over y, core).
Axes of the slice: x: 2, y: 2, z: 4, core: 2. Of those that a mesh axis runs over, the one named last changes fastest.
Arguments:
- state_blocks: bfloat16 [8, 512, 512], P('sec'), may hold values from -6 to 6
- left_blocks: bfloat16 [32, 8, 512, 512], P('chan', 'sec'), may hold values from -0.25 to 0.25
- right_blocks: bfloat16 [32, 8, 512, 512], P('chan', 'sec'), may hold values from -0.25 to 0.25
- widths: int32 [8], P('sec'), may hold values from 128 to 512
- step_sizes: float32 [8], P('sec'), may hold values from 0.1 to 0.4
- shifts: int32 [32], P('chan'), may hold values from -1 to 1
Outputs:
- update: bfloat16 [8, 512, 512], P('sec', 'chan')
- new_left: bfloat16 [32, 8, 512, 512], P('chan', 'sec')
The draws below stay inside these ranges and needn't reach their ends.
All inputs are finite; a program needn't handle non-finite values.
Results may differ from the reference program's by a relative error of at most 0.012.
Values may be sent and summed in bfloat16 or wider, within the bound.
No kernel may reach another device: no remote copies, remote signals or barrier semaphores. Data moves between devices by JAX's collectives and lax.ppermute only.
A program may use at most 64 MiB of HBM per device.

```python
import math
import jax
import jax.numpy as jnp
from jax import lax

PAD = 512
REACH = 1
SECTORS = 8
CHANNELS = 32


def plant(drawn, key, least, high):
    place = [jax.random.randint(jax.random.fold_in(key, axis), (), 0, length) for axis, length in enumerate(drawn.shape)]
    main_axis = drawn.shape.index(max(drawn.shape))
    beside = place[:main_axis] + [(place[main_axis] + 1) % drawn.shape[main_axis]] + place[main_axis + 1:]
    return drawn.at[tuple(place)].set(least).at[tuple(beside)].set(high)


def block_scale(key, shape, shards, low, high):
    factor_of = 1.0
    for axis_at, blocks in shards:
        draws = jax.random.uniform(jax.random.fold_in(jax.random.fold_in(key, 6), axis_at), (blocks,), jnp.float32, low / len(shards), high / len(shards))
        factor_of = factor_of * jnp.repeat(jnp.exp(draws), shape[axis_at] // blocks).reshape((-1,) + (1,) * (len(shape) - 1 - axis_at))
    return factor_of


def scatter_about(rng, shape, width, limit, split=(), kind=jnp.bfloat16):
    values = jax.random.normal(rng, shape, jnp.float32) * width
    if len(split) > 0:
        values = block_scale(rng, shape, split, -0.22, 0.18) * values
    return jnp.clip(values, min=-limit, max=limit).astype(kind)


def setup_inputs(seed: int = 0) -> dict:
    arg_keys = jax.random.split(jax.random.key(seed), 7)
    return {
        "state_blocks": scatter_about(arg_keys[0], (SECTORS, PAD, PAD), 1.0, 6.0, ((0, 8),)),
        "left_blocks": scatter_about(arg_keys[1], (CHANNELS, SECTORS, PAD, PAD), PAD ** -0.5, 0.25, ((0, 4), (1, 8))),
        "right_blocks": scatter_about(arg_keys[2], (CHANNELS, SECTORS, PAD, PAD), PAD ** -0.5, 0.25, ((0, 4), (1, 8))),
        "widths": plant(jax.random.randint(arg_keys[3], (SECTORS,), PAD // 4, PAD + 1), jax.random.fold_in(arg_keys[3], 1), PAD // 4, PAD).astype(jnp.int32),
        "step_sizes": jnp.clip(jnp.exp(math.log(0.4) - 1.3862944 * jax.random.uniform(arg_keys[4], (SECTORS,), jnp.float32) ** block_scale(arg_keys[4], (SECTORS,), ((0, 8),), -0.2, 0.2)), 0.1, 0.4),
        "shifts": plant(jax.random.randint(arg_keys[5], (CHANNELS,), -REACH, REACH + 1), jax.random.fold_in(arg_keys[5], 1), -REACH, REACH).astype(jnp.int32),
    }


def reference(state_blocks, left_blocks, right_blocks, widths, step_sizes, shifts):
    positions = jnp.arange(PAD, dtype=jnp.int32)
    within = positions[None, :] < widths[:, None]
    inside = within[:, :, None] & within[:, None, :]
    states = jnp.where(inside, state_blocks, jnp.zeros_like(state_blocks))
    sectors = jnp.arange(SECTORS, dtype=jnp.int32)

    def pick(blocks, offset):
        source = sectors - offset
        valid = (source >= 0) & (source < SECTORS)
        taken = blocks[jnp.clip(source, 0, SECTORS - 1).astype(jnp.int32)]
        return jnp.where(valid[:, None, None], taken, jnp.zeros_like(taken))

    def matvec_step(total, pieces):
        left, right, offset = pieces
        source = pick(states, offset)
        halfway = jnp.einsum("sab,sbd->sad", left.astype(jnp.float32), source.astype(jnp.float32)).astype(jnp.bfloat16)
        second = jnp.einsum("sad,sed->sae", halfway.astype(jnp.float32), right.astype(jnp.float32))
        return total + second, None

    total, _ = lax.scan(matvec_step, jnp.zeros((SECTORS, PAD, PAD), jnp.float32), (left_blocks, right_blocks, shifts))
    product_sum = jnp.where(inside, total, jnp.zeros_like(total))
    corrected = states.astype(jnp.float32) - step_sizes[:, None, None] * product_sum
    update = jnp.where(inside, corrected, jnp.zeros_like(corrected)).astype(jnp.bfloat16)

    def rotate(pieces):
        left, offset = pieces
        ket_block = pick(update, offset)
        pulled = jnp.einsum("sab,sby->say", left.astype(jnp.float32), ket_block.astype(jnp.float32)).astype(jnp.bfloat16)
        rotated = jnp.einsum("sax,say->sxy", update.astype(jnp.float32), pulled.astype(jnp.float32))
        return (rotated * (PAD ** -0.5)).astype(jnp.bfloat16)

    new_left = lax.map(rotate, (left_blocks, shifts))
    return update, new_left
```

```python
import functools

import jax
import jax.numpy as jnp
from jax import lax
from jax.experimental import pallas as pl
from jax.experimental.pallas import tpu as pltpu
from jax.sharding import PartitionSpec as P

BF16 = jnp.bfloat16
F32 = jnp.float32


def swap_core(x):
    count = lax.axis_size("chan")
    return lax.ppermute(x, "chan", [(i, i ^ 1) for i in range(count) if i ^ 1 < count])


def swap_near(x):
    count = lax.axis_size("sec")
    return lax.ppermute(x, "sec", [(i, i ^ 1) for i in range(count) if i ^ 1 < count])


def pass_far(x):
    count = lax.axis_size("sec")
    pairs = []
    for s in range(count):
        t = s + 2 if s % 2 == 0 else s - 2
        if 0 <= t < count and s ^ 1 < count:
            pairs.append((s, t))
    return lax.ppermute(x, "sec", pairs)


def join(dst, parity, mine, other, width):
    @pl.when(parity == 0)
    def _():
        dst[:, :width] = mine[...]
        dst[:, width:] = other[...]

    @pl.when(parity == 1)
    def _():
        dst[:, :width] = other[...]
        dst[:, width:] = mine[...]


def sum_kernel(scal, own, near_m, near_o, far_m, far_o, left, right, keep, give, src, acc):
    step = pl.program_id(0)
    last = pl.num_programs(0) - 1
    width = keep.shape[1]
    parity = scal[0]

    @pl.when(step == 0)
    def _():
        src[0] = own[...]
        join(src.at[1], parity, near_m, near_o, width)
        join(src.at[2], parity, far_m, far_o, width)
        acc[...] = jnp.zeros_like(acc)

    source = src[scal[1 + step]]
    halfway = jnp.dot(left[0, 0], source, preferred_element_type=F32).astype(BF16)
    acc[...] += lax.dot_general(
        halfway, right[0, 0], (((1,), (1,)), ((), ())), preferred_element_type=F32
    )

    @pl.when(step == last)
    def _():
        @pl.when(parity == 0)
        def _():
            keep[...] = acc[:, :width]
            give[...] = acc[:, width:].astype(BF16)

        @pl.when(parity == 1)
        def _():
            keep[...] = acc[:, width:]
            give[...] = acc[:, :width].astype(BF16)


def channel_sum(scal, own, near_m, near_o, far_m, far_o, left, right):
    chans, _, pad, _ = left.shape
    half = pad // 2
    whole = pl.BlockSpec((pad, pad), lambda c, s: (0, 0))
    part = pl.BlockSpec((pad, half), lambda c, s: (0, 0))
    block = pl.BlockSpec((1, 1, pad, pad), lambda c, s: (c, 0, 0, 0))
    return pl.pallas_call(
        sum_kernel,
        grid_spec=pltpu.PrefetchScalarGridSpec(
            num_scalar_prefetch=1,
            grid=(chans,),
            in_specs=[whole, part, part, part, part, block, block],
            out_specs=[part, part],
            scratch_shapes=[pltpu.VMEM((3, pad, pad), BF16), pltpu.VMEM((pad, pad), F32)],
        ),
        out_shape=[
            jax.ShapeDtypeStruct((pad, half), F32),
            jax.ShapeDtypeStruct((pad, half), BF16),
        ],
        cost_estimate=pl.CostEstimate(
            flops=chans * 4 * pad**3, transcendentals=0, bytes_accessed=chans * 4 * pad * pad
        ),
        name="channel_sum",
    )(scal, own, near_m, near_o, far_m, far_o, left, right)


def rotate_kernel(scal, own_m, own_o, near_m, near_o, far_m, far_o, left, rows, new_left, src, bra):
    step = pl.program_id(0)
    width = own_m.shape[1]
    parity = scal[0]
    pad = src.shape[1]

    @pl.when(step == 0)
    def _():
        join(src.at[0], parity, own_m, own_o, width)
        join(src.at[1], parity, near_m, near_o, width)
        join(src.at[2], parity, far_m, far_o, width)
        bra[...] = src[0].T
        count = rows.shape[0]
        rows[...] = src[0, pl.ds(pl.multiple_of(scal[1] * count, count), count), :]

    ket = src[scal[2 + step]]
    pulled = jnp.dot(left[0, 0], ket, preferred_element_type=F32).astype(BF16)
    rotated = jnp.dot(bra[...], pulled, preferred_element_type=F32)
    new_left[0, 0] = (rotated * pad ** (-0.5)).astype(BF16)


def rotate(scal, own_m, own_o, near_m, near_o, far_m, far_o, left, share):
    chans, _, pad, _ = left.shape
    half = pad // 2
    part = pl.BlockSpec((pad, half), lambda c, s: (0, 0))
    block = pl.BlockSpec((1, 1, pad, pad), lambda c, s: (c, 0, 0, 0))
    return pl.pallas_call(
        rotate_kernel,
        grid_spec=pltpu.PrefetchScalarGridSpec(
            num_scalar_prefetch=1,
            grid=(chans,),
            in_specs=[part] * 6 + [block],
            out_specs=[pl.BlockSpec((share, pad), lambda c, s: (0, 0)), block],
            scratch_shapes=[pltpu.VMEM((3, pad, pad), BF16), pltpu.VMEM((pad, pad), BF16)],
        ),
        out_shape=[
            jax.ShapeDtypeStruct((share, pad), BF16),
            jax.ShapeDtypeStruct(left.shape, BF16),
        ],
        cost_estimate=pl.CostEstimate(
            flops=chans * 4 * pad**3, transcendentals=0, bytes_accessed=chans * 4 * pad * pad
        ),
        name="rotate",
    )(scal, own_m, own_o, near_m, near_o, far_m, far_o, left)


def shards(state_blocks, left_blocks, right_blocks, widths, step_sizes, shifts):
    pad = state_blocks.shape[1]
    half = pad // 2
    chan_count = lax.axis_size("chan")
    rank = lax.axis_index("chan")
    sector = lax.axis_index("sec")
    parity = rank % 2
    first = parity * half
    width = widths[0]
    positions = jnp.arange(pad, dtype=jnp.int32)
    within = positions < width
    inside = within[:, None] & within[None, :]
    states = jnp.where(inside, state_blocks[0], jnp.zeros_like(state_blocks[0]))
    states_m = lax.dynamic_slice_in_dim(states, first, half, 1)
    inside_m = lax.dynamic_slice_in_dim(inside, first, half, 1)

    near_offset = jnp.where(sector % 2 == 0, -1, 1)
    which = jnp.where(shifts == 0, 0, jnp.where(shifts == near_offset, 1, 2))

    near_m = swap_near(states_m)
    far_m = pass_far(near_m)
    near_o = swap_core(near_m)
    far_o = swap_core(far_m)
    scal = jnp.concatenate([parity[None], which]).astype(jnp.int32)
    keep, give = channel_sum(scal, states, near_m, near_o, far_m, far_o, left_blocks, right_blocks)
    pair_sum = (keep + swap_core(give).astype(F32)).astype(BF16)
    total = pair_sum.astype(F32)
    for turn in range(2, chan_count, 2):
        moved = lax.ppermute(
            pair_sum, "chan", [(i, (i + turn) % chan_count) for i in range(chan_count)]
        )
        total = total + moved.astype(F32)
    product = jnp.where(inside_m, total, jnp.zeros_like(total))
    corrected = states_m.astype(F32) - step_sizes[0] * product
    update_m = jnp.where(inside_m, corrected, jnp.zeros_like(corrected)).astype(BF16)

    unear_m = swap_near(update_m)
    ufar_m = pass_far(unear_m)
    update_o = swap_core(update_m)
    unear_o = swap_core(unear_m)
    ufar_o = swap_core(ufar_m)
    scal = jnp.concatenate([parity[None], rank[None], which]).astype(jnp.int32)
    rows, new_left = rotate(
        scal, update_m, update_o, unear_m, unear_o, ufar_m, ufar_o, left_blocks, pad // chan_count
    )
    return rows[None], new_left


def solution(mesh):
    placed = (
        P("sec", None, None),
        P("chan", "sec", None, None),
        P("chan", "sec", None, None),
        P("sec"),
        P("sec"),
        P("chan"),
    )
    return jax.shard_map(
        shards,
        mesh=mesh,
        in_specs=placed,
        out_specs=(P("sec", "chan", None), P("chan", "sec", None, None)),
        check_vma=False,
    )
```

```python
import functools

import jax
import jax.numpy as jnp
from jax import lax
from jax.experimental import pallas as pl
from jax.experimental.pallas import tpu as pltpu
from jax.sharding import PartitionSpec as P


BF16 = jnp.bfloat16
F32 = jnp.float32
OWN, NEAR, FAR = 0, 1, 2
ROOM = 28 << 20
VMEM = pl.BlockSpec(memory_space=pltpu.VMEM)
SMEM = pl.BlockSpec(memory_space=pltpu.SMEM)
ANY = pl.BlockSpec(memory_space=pl.ANY)


def held(x):
    return pltpu.with_memory_space_constraint(x, pltpu.VMEM)


def swap_core(x):
    count = lax.axis_size("chan")
    return lax.ppermute(x, "chan", [(i, i ^ 1) for i in range(count) if i ^ 1 < count])


def swap_near(x):
    count = lax.axis_size("sec")
    return lax.ppermute(x, "sec", [(i, i ^ 1) for i in range(count) if i ^ 1 < count])


def pass_far(x):
    count = lax.axis_size("sec")
    pairs = [(s, s + 2 if s % 2 == 0 else s - 2) for s in range(count)]
    pairs = [(s, t) for s, t in pairs if 0 <= t < count]
    sources = sorted(set(range(count)) - {s for s, _ in pairs})
    targets = sorted(set(range(count)) - {t for _, t in pairs})
    return lax.ppermute(x, "sec", pairs + list(zip(sources, targets)))


def far_exists():
    sector = lax.axis_index("sec")
    far = sector + 1 - 2 * lax.rem(sector + 1, 2)
    return (far >= 0) & (far < lax.axis_size("sec"))


def place(offset):
    near = 2 * lax.rem(lax.axis_index("sec"), 2) - 1
    return jnp.where(offset == 0, OWN, jnp.where(offset == near, NEAR, FAR))


def list_channels(shifts, order, wanted, start=0):
    count = jnp.int32(start)
    for channel in range(shifts.shape[0]):
        order[count] = channel
        count += jnp.where(place(shifts[channel]) == wanted, 1, 0)
    return count


def join(dst, mine, other, valid=None):
    parity = lax.rem(lax.axis_index("chan"), 2)
    half = mine.shape[0]
    dst[pl.ds(pl.multiple_of(parity * half, half), half), :] = mine[...]
    dst[pl.ds(pl.multiple_of((1 - parity) * half, half), half), :] = other[...]
    if valid is not None:

        @pl.when(jnp.logical_not(valid))
        def _():
            dst[...] = jnp.zeros_like(dst)


def add_terms(count, order, src, left, right, acc, ready):
    def body(i, carry):
        channel = order[i]
        ready(channel)
        halfway = jnp.dot(left[channel], src[...], preferred_element_type=F32).astype(BF16)
        acc[...] += lax.dot_general(
            halfway, right[channel], (((1,), (1,)), ((), ())), preferred_element_type=F32
        )
        return carry

    lax.fori_loop(0, count, body, 0)


def own_sum_kernel(
    shifts_in, widths_in, state_in, left_in, right_in, acc, left, right,
    src, shifts, widths, order, small_sem, left_sem, right_sem
):
    small = [
        pltpu.make_async_copy(shifts_in, shifts, small_sem.at[0]),
        pltpu.make_async_copy(widths_in, widths, small_sem.at[1]),
        pltpu.make_async_copy(state_in.at[0], src, small_sem.at[2]),
    ]
    for copy in small:
        copy.start()

    def loads(channel):
        return (
            pltpu.make_async_copy(left_in.at[channel, 0], left.at[channel], left_sem.at[channel]),
            pltpu.make_async_copy(right_in.at[channel, 0], right.at[channel], right_sem.at[channel]),
        )

    small[0].wait()
    owned = list_channels(shifts, order, OWN)
    near = list_channels(shifts, order, NEAR, owned)
    list_channels(shifts, order, FAR, near)

    def fetch(i, carry):
        for copy in loads(order[i]):
            copy.start()
        return carry

    lax.fori_loop(0, left.shape[0], fetch, 0)
    acc[...] = jnp.zeros_like(acc)
    small[1].wait()
    small[2].wait()
    rows = lax.broadcasted_iota(jnp.int32, src.shape, 0)
    cols = lax.broadcasted_iota(jnp.int32, src.shape, 1)
    inside = (rows < widths[0]) & (cols < widths[0])
    src[...] = jnp.where(inside, src[...], jnp.zeros_like(src))

    def ready(channel):
        for copy in loads(channel):
            copy.wait()

    add_terms(owned, order, src, left, right, acc, ready)

    def rest(i, carry):
        ready(order[i])
        return carry

    lax.fori_loop(owned, left.shape[0], rest, 0)


def next_sum_kernel(wanted, last, shifts, mine, other, acc_in, left, right, *rest):
    if last:
        keep, give, acc, src, order = rest
    else:
        acc, src, order = rest
    count = list_channels(shifts, order, wanted)
    join(src, mine, other, far_exists() if last else None)
    acc[...] = acc_in[...]
    add_terms(count, order, src, left, right, acc, lambda channel: None)
    if last:
        half = keep.shape[0]
        parity = lax.rem(lax.axis_index("chan"), 2)
        keep[...] = acc[pl.ds(pl.multiple_of(parity * half, half), half), :]
        give[...] = acc[pl.ds(pl.multiple_of((1 - parity) * half, half), half), :].astype(BF16)


def cost(matmuls, pad):
    return pl.CostEstimate(
        flops=int(matmuls * 2 * pad**3), transcendentals=0, bytes_accessed=int(matmuls * 2 * pad**2)
    )


def own_sum(shifts, widths, state, left, right):
    chans, _, pad, _ = left.shape
    blocks = jax.ShapeDtypeStruct((chans, pad, pad), BF16)
    return pl.pallas_call(
        own_sum_kernel,
        in_specs=[ANY] * 5,
        out_specs=[VMEM] * 3,
        out_shape=[jax.ShapeDtypeStruct((pad, pad), F32), blocks, blocks],
        scratch_shapes=[
            pltpu.VMEM((pad, pad), BF16),
            pltpu.SMEM(shifts.shape, jnp.int32),
            pltpu.SMEM(widths.shape, jnp.int32),
            pltpu.SMEM((chans + 1,), jnp.int32),
            pltpu.SemaphoreType.DMA((3,)),
            pltpu.SemaphoreType.DMA((chans,)),
            pltpu.SemaphoreType.DMA((chans,)),
        ],
        compiler_params=pltpu.CompilerParams(vmem_limit_bytes=ROOM),
        cost_estimate=cost(2 * chans / 3, pad),
        name="own_sum",
    )(shifts, widths, *[pltpu.with_memory_space_constraint(x, pltpu.HBM) for x in (state, left, right)])


def next_sum(wanted, last, shifts, mine, other, acc, left, right):
    chans, pad, _ = left.shape
    half = pad // 2
    whole = jax.ShapeDtypeStruct((pad, pad), F32)
    scratch = [pltpu.VMEM((pad, pad), BF16), pltpu.SMEM((chans + 1,), jnp.int32)]
    if last:
        scratch = [pltpu.VMEM((pad, pad), F32)] + scratch
    return pl.pallas_call(
        functools.partial(next_sum_kernel, wanted, last),
        in_specs=[SMEM] + [VMEM] * 5,
        out_specs=[VMEM, VMEM] if last else VMEM,
        out_shape=[
            jax.ShapeDtypeStruct((half, pad), F32),
            jax.ShapeDtypeStruct((half, pad), BF16),
        ]
        if last
        else whole,
        scratch_shapes=scratch,
        compiler_params=pltpu.CompilerParams(vmem_limit_bytes=ROOM),
        cost_estimate=cost(2 * chans / 3, pad),
        name="far_sum" if last else "near_sum",
    )(shifts, *[held(x) for x in (mine, other, acc, left, right)])


def finish(first, count, order, turned, src, new_left, obuf, osem, ready=None):
    scale = src.shape[0] ** (-0.5)

    def store(i):
        return pltpu.make_async_copy(obuf.at[i], new_left.at[order[i], 0], osem.at[i])

    def body(i, carry):
        bra_left = ready[i] if turned is None else turned(order[i])
        rotated = jnp.dot(bra_left, src[...], preferred_element_type=F32)
        obuf[i] = (rotated * scale).astype(BF16)
        store(i).start()
        return carry

    lax.fori_loop(first, count, body, 0)

    def drain(i, carry):
        store(i).wait()
        return carry

    return lambda: lax.fori_loop(first, count, drain, 0)


def turn(bra, left, channel):
    return jnp.dot(bra[...], left[channel], preferred_element_type=F32).astype(BF16)


def turn_ahead(shifts, order, wanted, bra, left, half_turned):
    count = list_channels(shifts, order, wanted)

    def body(i, carry):
        half_turned[i] = turn(bra, left, order[i])
        return carry

    lax.fori_loop(0, count, body, 0)


def own_turn_kernel(
    shifts, mine, other, left, rows, new_left, half_turned, bra, src, order, ahead, obuf, osem
):
    owned = list_channels(shifts, order, OWN)
    join(src, mine, other)
    bra[...] = src[...].T
    share = rows.shape[0]
    rows[...] = src[pl.ds(pl.multiple_of(lax.axis_index("chan") * share, share), share), :]
    drain = finish(
        0, owned, order, lambda channel: turn(bra, left, channel), src, new_left, obuf, osem
    )
    turn_ahead(shifts, ahead, NEAR, bra, left, half_turned)
    drain()


def turn_scratch(chans, pad):
    return [
        pltpu.VMEM((pad, pad), BF16),
        pltpu.SMEM((chans + 1,), jnp.int32),
        pltpu.SMEM((chans + 1,), jnp.int32),
        pltpu.VMEM((chans, pad, pad), BF16),
        pltpu.SemaphoreType.DMA((chans,)),
    ]


def own_turn(shifts, mine, other, left, share):
    chans, pad, _ = left.shape
    return pl.pallas_call(
        own_turn_kernel,
        in_specs=[SMEM, VMEM, VMEM, VMEM],
        out_specs=[VMEM, ANY, VMEM, VMEM],
        out_shape=[
            jax.ShapeDtypeStruct((share, pad), BF16),
            jax.ShapeDtypeStruct((chans, 1, pad, pad), BF16),
            jax.ShapeDtypeStruct((chans, pad, pad), BF16),
            jax.ShapeDtypeStruct((pad, pad), BF16),
        ],
        scratch_shapes=turn_scratch(chans, pad),
        compiler_params=pltpu.CompilerParams(vmem_limit_bytes=ROOM),
        cost_estimate=cost(chans, pad),
        name="own_turn",
    )(shifts, held(mine), held(other), held(left))


def near_turn_kernel(
    shifts, mine, other, half_turned, bra, left, old, new_left, far_turned, src, order, ahead, obuf, osem
):
    count = list_channels(shifts, order, NEAR)
    join(src, mine, other)
    drain = finish(0, count, order, None, src, new_left, obuf, osem, half_turned)
    turn_ahead(shifts, ahead, FAR, bra, left, far_turned)
    drain()


def near_turn(shifts, mine, other, half_turned, bra, left, new_left):
    chans, pad, _ = left.shape
    return pl.pallas_call(
        near_turn_kernel,
        in_specs=[SMEM] + [VMEM] * 5 + [ANY],
        out_specs=[ANY, VMEM],
        out_shape=[
            jax.ShapeDtypeStruct(new_left.shape, BF16),
            jax.ShapeDtypeStruct((chans, pad, pad), BF16),
        ],
        scratch_shapes=turn_scratch(chans, pad),
        input_output_aliases={6: 0},
        compiler_params=pltpu.CompilerParams(vmem_limit_bytes=ROOM),
        cost_estimate=cost(2 * chans / 3, pad),
        name="near_turn",
    )(shifts, *[held(x) for x in (mine, other, half_turned, bra, left)], new_left)


def far_turn_kernel(shifts, mine, other, far_turned, old, new_left, src, order, ahead, obuf, osem):
    count = list_channels(shifts, order, FAR)
    join(src, mine, other, far_exists())
    finish(0, count, order, None, src, new_left, obuf, osem, far_turned)()


def far_turn(shifts, mine, other, far_turned, new_left):
    chans, pad, _ = far_turned.shape
    return pl.pallas_call(
        far_turn_kernel,
        in_specs=[SMEM] + [VMEM] * 3 + [ANY],
        out_specs=ANY,
        out_shape=jax.ShapeDtypeStruct(new_left.shape, BF16),
        scratch_shapes=turn_scratch(chans, pad),
        input_output_aliases={4: 0},
        compiler_params=pltpu.CompilerParams(vmem_limit_bytes=ROOM),
        cost_estimate=cost(chans / 3, pad),
        name="far_turn",
    )(shifts, held(mine), held(other), held(far_turned), new_left)


def exchange(mine):
    near_a = swap_near(mine[: mine.shape[0] // 2])
    near_b = swap_near(mine[mine.shape[0] // 2 :])
    far_a = pass_far(near_a)
    far_b = pass_far(near_b)
    near = held(jnp.concatenate([near_a, near_b]))
    far = held(jnp.concatenate([far_a, far_b]))
    near_other = swap_core(near)
    far_other = swap_core(far)
    return near, near_other, far, far_other


def body(state_blocks, left_blocks, right_blocks, widths, step_sizes, shifts):
    pad = state_blocks.shape[1]
    half = pad // 2
    chan_count = lax.axis_size("chan")
    first = lax.axis_index("chan") % 2 * half
    width = widths[0]
    positions = jnp.arange(pad, dtype=jnp.int32)
    inside = ((first + positions[:half]) < width)[:, None] & (positions < width)[None, :]
    state_m = lax.dynamic_slice_in_dim(state_blocks[0], first, half, 0)
    state_m = jnp.where(inside, state_m, jnp.zeros_like(state_m))

    near_m, near_o, far_m, far_o = exchange(state_m)
    acc, left, right = own_sum(shifts, widths, state_blocks, left_blocks, right_blocks)
    acc = next_sum(NEAR, False, shifts, near_m, near_o, acc, left, right)
    keep, give = next_sum(FAR, True, shifts, far_m, far_o, acc, left, right)

    pair_sum = (keep + swap_core(give).astype(F32)).astype(BF16)
    total = pair_sum.astype(F32)
    for turn in range(2, chan_count, 2):
        moved = lax.ppermute(
            pair_sum, "chan", [(i, (i + turn) % chan_count) for i in range(chan_count)]
        )
        total = total + moved.astype(F32)
    product = jnp.where(inside, total, jnp.zeros_like(total))
    corrected = state_m.astype(F32) - step_sizes[0] * product
    update_m = jnp.where(inside, corrected, jnp.zeros_like(corrected)).astype(BF16)

    near_m, near_o, far_m, far_o = exchange(update_m)
    update_o = swap_core(update_m)
    rows, new_left, half_turned, bra = own_turn(shifts, update_m, update_o, left, pad // chan_count)
    new_left, far_turned = near_turn(
        shifts, near_m, near_o, half_turned, bra, left, new_left
    )
    new_left = far_turn(shifts, far_m, far_o, far_turned, new_left)
    return rows[None], new_left


def solution(mesh):
    placed = (
        P("sec", None, None),
        P("chan", "sec", None, None),
        P("chan", "sec", None, None),
        P("sec"),
        P("sec"),
        P("chan"),
    )
    return jax.shard_map(
        body,
        mesh=mesh,
        in_specs=placed,
        out_specs=(P("sec", "chan", None), P("chan", "sec", None, None)),
        check_vma=False,
    )
```

```python
import functools

import jax
import jax.numpy as jnp
from jax import lax
from jax.experimental import pallas as pl
from jax.experimental.pallas import tpu as pltpu
from jax.sharding import PartitionSpec as P


BF16 = jnp.bfloat16
F32 = jnp.float32
OWN, NEAR, FAR = 0, 1, 2
ROOM = 28 << 20
VMEM = pl.BlockSpec(memory_space=pltpu.VMEM)
SMEM = pl.BlockSpec(memory_space=pltpu.SMEM)
ANY = pl.BlockSpec(memory_space=pl.ANY)


def held(x):
    return pltpu.with_memory_space_constraint(x, pltpu.VMEM)


def swap_core(x):
    count = lax.axis_size("chan")
    return lax.ppermute(x, "chan", [(i, i ^ 1) for i in range(count) if i ^ 1 < count])


def swap_near(x):
    count = lax.axis_size("sec")
    return lax.ppermute(x, "sec", [(i, i ^ 1) for i in range(count) if i ^ 1 < count])


def pass_far(x):
    count = lax.axis_size("sec")
    pairs = [(s, s + 2 if s % 2 == 0 else s - 2) for s in range(count)]
    pairs = [(s, t) for s, t in pairs if 0 <= t < count]
    sources = sorted(set(range(count)) - {s for s, _ in pairs})
    targets = sorted(set(range(count)) - {t for _, t in pairs})
    return lax.ppermute(x, "sec", pairs + list(zip(sources, targets)))


def far_exists():
    sector = lax.axis_index("sec")
    far = sector + 1 - 2 * lax.rem(sector + 1, 2)
    return (far >= 0) & (far < lax.axis_size("sec"))


def place(offset):
    near = 2 * lax.rem(lax.axis_index("sec"), 2) - 1
    return jnp.where(offset == 0, OWN, jnp.where(offset == near, NEAR, FAR))


def list_channels(shifts, order, wanted, start=0):
    count = jnp.int32(start)
    for channel in range(shifts.shape[0]):
        order[count] = channel
        count += jnp.where(place(shifts[channel]) == wanted, 1, 0)
    return count


def join(dst, mine, other, valid=None):
    parity = lax.rem(lax.axis_index("chan"), 2)
    half = mine.shape[0]
    dst[pl.ds(pl.multiple_of(parity * half, half), half), :] = mine[...]
    dst[pl.ds(pl.multiple_of((1 - parity) * half, half), half), :] = other[...]
    if valid is not None:

        @pl.when(jnp.logical_not(valid))
        def _():
            dst[...] = jnp.zeros_like(dst)


def by_twos(first, count, step):
    pairs = lax.div(count - first, 2)

    def body(i, carry):
        step(first + 2 * i, 2)
        return carry

    lax.fori_loop(0, pairs, body, 0)

    @pl.when(count - first > 2 * pairs)
    def _():
        step(count - 1, 1)


def add_terms(count, order, src, left, right, acc, ready):
    def step(i, n):
        channels = [order[i + j] for j in range(n)]
        for channel in channels:
            ready(channel)
        halfway = [
            jnp.dot(left[channel], src[...], preferred_element_type=F32).astype(BF16)
            for channel in channels
        ]
        terms = [
            lax.dot_general(h, right[channel], (((1,), (1,)), ((), ())), preferred_element_type=F32)
            for h, channel in zip(halfway, channels)
        ]
        acc[...] += sum(terms[1:], terms[0])

    by_twos(0, count, step)


def own_sum_kernel(
    shifts_in, widths_in, state_in, left_in, right_in, acc, left, right, shifts,
    src, widths, order, small_sem, left_sem, right_sem
):
    small = [
        pltpu.make_async_copy(shifts_in, shifts, small_sem.at[0]),
        pltpu.make_async_copy(widths_in, widths, small_sem.at[1]),
        pltpu.make_async_copy(state_in.at[0], src, small_sem.at[2]),
    ]
    for copy in small:
        copy.start()

    def loads(channel):
        return (
            pltpu.make_async_copy(left_in.at[channel, 0], left.at[channel], left_sem.at[channel]),
            pltpu.make_async_copy(right_in.at[channel, 0], right.at[channel], right_sem.at[channel]),
        )

    small[0].wait()
    owned = list_channels(shifts, order, OWN)
    near = list_channels(shifts, order, NEAR, owned)
    list_channels(shifts, order, FAR, near)

    def fetch(i, carry):
        for copy in loads(order[i]):
            copy.start()
        return carry

    lax.fori_loop(0, left.shape[0], fetch, 0)
    acc[...] = jnp.zeros_like(acc)
    small[1].wait()
    small[2].wait()
    rows = lax.broadcasted_iota(jnp.int32, src.shape, 0)
    cols = lax.broadcasted_iota(jnp.int32, src.shape, 1)
    inside = (rows < widths[0]) & (cols < widths[0])
    src[...] = jnp.where(inside, src[...], jnp.zeros_like(src))

    def ready(channel):
        for copy in loads(channel):
            copy.wait()

    add_terms(owned, order, src, left, right, acc, ready)

    def rest(i, carry):
        ready(order[i])
        return carry

    lax.fori_loop(owned, left.shape[0], rest, 0)


def next_sum_kernel(wanted, last, shifts, mine, other, acc_in, left, right, *rest):
    if last:
        keep, give, acc, src, order = rest
    else:
        acc, src, order = rest
    count = list_channels(shifts, order, wanted)
    join(src, mine, other, far_exists() if last else None)
    acc[...] = acc_in[...]
    add_terms(count, order, src, left, right, acc, lambda channel: None)
    if last:
        half = keep.shape[0]
        parity = lax.rem(lax.axis_index("chan"), 2)
        keep[...] = acc[pl.ds(pl.multiple_of(parity * half, half), half), :]
        give[...] = acc[pl.ds(pl.multiple_of((1 - parity) * half, half), half), :].astype(BF16)


def cost(matmuls, pad):
    return pl.CostEstimate(
        flops=int(matmuls * 2 * pad**3), transcendentals=0, bytes_accessed=int(matmuls * 2 * pad**2)
    )


def own_sum(shifts, widths, state, left, right):
    chans, _, pad, _ = left.shape
    blocks = jax.ShapeDtypeStruct((chans, pad, pad), BF16)
    return pl.pallas_call(
        own_sum_kernel,
        in_specs=[ANY] * 5,
        out_specs=[VMEM] * 3 + [SMEM],
        out_shape=[
            jax.ShapeDtypeStruct((pad, pad), F32),
            blocks,
            blocks,
            jax.ShapeDtypeStruct(shifts.shape, jnp.int32),
        ],
        scratch_shapes=[
            pltpu.VMEM((pad, pad), BF16),
            pltpu.SMEM(widths.shape, jnp.int32),
            pltpu.SMEM((chans + 1,), jnp.int32),
            pltpu.SemaphoreType.DMA((3,)),
            pltpu.SemaphoreType.DMA((chans,)),
            pltpu.SemaphoreType.DMA((chans,)),
        ],
        compiler_params=pltpu.CompilerParams(vmem_limit_bytes=ROOM),
        cost_estimate=cost(2 * chans / 3, pad),
        name="own_sum",
    )(shifts, widths, *[pltpu.with_memory_space_constraint(x, pltpu.HBM) for x in (state, left, right)])


def next_sum(wanted, last, shifts, mine, other, acc, left, right):
    chans, pad, _ = left.shape
    half = pad // 2
    whole = jax.ShapeDtypeStruct((pad, pad), F32)
    scratch = [pltpu.VMEM((pad, pad), BF16), pltpu.SMEM((chans + 1,), jnp.int32)]
    if last:
        scratch = [pltpu.VMEM((pad, pad), F32)] + scratch
    return pl.pallas_call(
        functools.partial(next_sum_kernel, wanted, last),
        in_specs=[SMEM] + [VMEM] * 5,
        out_specs=[VMEM, VMEM] if last else VMEM,
        out_shape=[
            jax.ShapeDtypeStruct((half, pad), F32),
            jax.ShapeDtypeStruct((half, pad), BF16),
        ]
        if last
        else whole,
        scratch_shapes=scratch,
        compiler_params=pltpu.CompilerParams(vmem_limit_bytes=ROOM),
        cost_estimate=cost(2 * chans / 3, pad),
        name="far_sum" if last else "near_sum",
    )(shifts, *[held(x) for x in (mine, other, acc, left, right)])


def finish(first, count, order, turned, src, new_left, obuf, osem, ready=None):
    scale = src.shape[0] ** (-0.5)

    def store(i):
        return pltpu.make_async_copy(obuf.at[i], new_left.at[order[i], 0], osem.at[i])

    def step(i, n):
        slots = [i + j for j in range(n)]
        bra_left = [ready[k] if turned is None else turned(order[k]) for k in slots]
        rotated = [jnp.dot(x, src[...], preferred_element_type=F32) for x in bra_left]
        for k, x in zip(slots, rotated):
            obuf[k] = (x * scale).astype(BF16)
            store(k).start()

    by_twos(first, count, step)

    def drain(i, carry):
        store(i).wait()
        return carry

    return lambda: lax.fori_loop(first, count, drain, 0)


def turn(bra, left, channel):
    return jnp.dot(bra[...], left[channel], preferred_element_type=F32).astype(BF16)


def turn_ahead(shifts, order, wanted, bra, left, half_turned):
    count = list_channels(shifts, order, wanted)

    def step(i, n):
        for k, x in [(i + j, turn(bra, left, order[i + j])) for j in range(n)]:
            half_turned[k] = x

    by_twos(0, count, step)


def own_turn_kernel(
    shifts, mine, other, left, rows, new_left, half_turned, bra, src, order, ahead, obuf, osem
):
    owned = list_channels(shifts, order, OWN)
    join(src, mine, other)
    bra[...] = src[...].T
    share = rows.shape[0]
    rows[...] = src[pl.ds(pl.multiple_of(lax.axis_index("chan") * share, share), share), :]
    drain = finish(
        0, owned, order, lambda channel: turn(bra, left, channel), src, new_left, obuf, osem
    )
    turn_ahead(shifts, ahead, NEAR, bra, left, half_turned)
    drain()


def turn_scratch(chans, pad):
    return [
        pltpu.VMEM((pad, pad), BF16),
        pltpu.SMEM((chans + 1,), jnp.int32),
        pltpu.SMEM((chans + 1,), jnp.int32),
        pltpu.VMEM((chans, pad, pad), BF16),
        pltpu.SemaphoreType.DMA((chans,)),
    ]


def own_turn(shifts, mine, other, left, share):
    chans, pad, _ = left.shape
    return pl.pallas_call(
        own_turn_kernel,
        in_specs=[SMEM, VMEM, VMEM, VMEM],
        out_specs=[VMEM, ANY, VMEM, VMEM],
        out_shape=[
            jax.ShapeDtypeStruct((share, pad), BF16),
            jax.ShapeDtypeStruct((chans, 1, pad, pad), BF16),
            jax.ShapeDtypeStruct((chans, pad, pad), BF16),
            jax.ShapeDtypeStruct((pad, pad), BF16),
        ],
        scratch_shapes=turn_scratch(chans, pad),
        compiler_params=pltpu.CompilerParams(vmem_limit_bytes=ROOM),
        cost_estimate=cost(chans, pad),
        name="own_turn",
    )(shifts, held(mine), held(other), held(left))


def near_turn_kernel(
    shifts, mine, other, half_turned, bra, left, old, new_left, far_turned, src, order, ahead, obuf, osem
):
    count = list_channels(shifts, order, NEAR)
    join(src, mine, other)
    drain = finish(0, count, order, None, src, new_left, obuf, osem, half_turned)
    turn_ahead(shifts, ahead, FAR, bra, left, far_turned)
    drain()


def near_turn(shifts, mine, other, half_turned, bra, left, new_left):
    chans, pad, _ = left.shape
    return pl.pallas_call(
        near_turn_kernel,
        in_specs=[SMEM] + [VMEM] * 5 + [ANY],
        out_specs=[ANY, VMEM],
        out_shape=[
            jax.ShapeDtypeStruct(new_left.shape, BF16),
            jax.ShapeDtypeStruct((chans, pad, pad), BF16),
        ],
        scratch_shapes=turn_scratch(chans, pad),
        input_output_aliases={6: 0},
        compiler_params=pltpu.CompilerParams(vmem_limit_bytes=ROOM),
        cost_estimate=cost(2 * chans / 3, pad),
        name="near_turn",
    )(shifts, *[held(x) for x in (mine, other, half_turned, bra, left)], new_left)


def far_turn_kernel(shifts, mine, other, far_turned, old, new_left, src, order, ahead, obuf, osem):
    count = list_channels(shifts, order, FAR)
    join(src, mine, other, far_exists())
    finish(0, count, order, None, src, new_left, obuf, osem, far_turned)()


def far_turn(shifts, mine, other, far_turned, new_left):
    chans, pad, _ = far_turned.shape
    return pl.pallas_call(
        far_turn_kernel,
        in_specs=[SMEM] + [VMEM] * 3 + [ANY],
        out_specs=ANY,
        out_shape=jax.ShapeDtypeStruct(new_left.shape, BF16),
        scratch_shapes=turn_scratch(chans, pad),
        input_output_aliases={4: 0},
        compiler_params=pltpu.CompilerParams(vmem_limit_bytes=ROOM),
        cost_estimate=cost(chans / 3, pad),
        name="far_turn",
    )(shifts, held(mine), held(other), held(far_turned), new_left)


def exchange(mine, chunks):
    rows = mine.shape[0] // chunks
    near, far = [], []
    for i in range(chunks):
        near.append(swap_near(mine[i * rows : (i + 1) * rows]))
    for i in range(chunks):
        far.append(pass_far(near[i]))
    near = held(jnp.concatenate(near))
    far = held(jnp.concatenate(far))
    near_other = swap_core(near)
    far_other = swap_core(far)
    return near, near_other, far, far_other


def body(state_blocks, left_blocks, right_blocks, widths, step_sizes, shifts):
    pad = state_blocks.shape[1]
    half = pad // 2
    chan_count = lax.axis_size("chan")
    first = lax.axis_index("chan") % 2 * half
    width = widths[0]
    positions = jnp.arange(pad, dtype=jnp.int32)
    inside = ((first + positions[:half]) < width)[:, None] & (positions < width)[None, :]
    state_m = lax.dynamic_slice_in_dim(state_blocks[0], first, half, 0)
    state_m = jnp.where(inside, state_m, jnp.zeros_like(state_m))

    near_m, near_o, far_m, far_o = exchange(state_m, 2)
    acc, left, right, shifts = own_sum(shifts, widths, state_blocks, left_blocks, right_blocks)
    acc = next_sum(NEAR, False, shifts, near_m, near_o, acc, left, right)
    keep, give = next_sum(FAR, True, shifts, far_m, far_o, acc, left, right)

    pair_sum = (keep + swap_core(give).astype(F32)).astype(BF16)
    total = pair_sum.astype(F32)
    for turn in range(2, chan_count, 2):
        moved = lax.ppermute(
            pair_sum, "chan", [(i, (i + turn) % chan_count) for i in range(chan_count)]
        )
        total = total + moved.astype(F32)
    product = jnp.where(inside, total, jnp.zeros_like(total))
    corrected = state_m.astype(F32) - step_sizes[0] * product
    update_m = jnp.where(inside, corrected, jnp.zeros_like(corrected)).astype(BF16)

    near_m, near_o, far_m, far_o = exchange(update_m, 1)
    update_o = swap_core(update_m)
    rows, new_left, half_turned, bra = own_turn(shifts, update_m, update_o, left, pad // chan_count)
    new_left, far_turned = near_turn(
        shifts, near_m, near_o, half_turned, bra, left, new_left
    )
    new_left = far_turn(shifts, far_m, far_o, far_turned, new_left)
    return rows[None], new_left


def solution(mesh):
    placed = (
        P("sec", None, None),
        P("chan", "sec", None, None),
        P("chan", "sec", None, None),
        P("sec"),
        P("sec"),
        P("chan"),
    )
    return jax.shard_map(
        body,
        mesh=mesh,
        in_specs=placed,
        out_specs=(P("sec", "chan", None), P("chan", "sec", None, None)),
        check_vma=False,
    )
```

```python
import jax
import jax.numpy as jnp
from jax import lax
from jax.experimental import pallas as pl
from jax.experimental.pallas import tpu as pltpu
from jax.sharding import PartitionSpec as P


BF16 = jnp.bfloat16
F32 = jnp.float32
OWN, NEAR, FAR = 0, 1, 2
ROOM = 28 << 20
VMEM = pl.BlockSpec(memory_space=pltpu.VMEM)
SMEM = pl.BlockSpec(memory_space=pltpu.SMEM)
ANY = pl.BlockSpec(memory_space=pl.ANY)


def held(x):
    return pltpu.with_memory_space_constraint(x, pltpu.VMEM)


def in_hbm(x):
    return pltpu.with_memory_space_constraint(x, pltpu.HBM)


def swap_core(x):
    count = lax.axis_size("chan")
    return lax.ppermute(x, "chan", [(i, i ^ 1) for i in range(count) if i ^ 1 < count])


def swap_near(x):
    count = lax.axis_size("sec")
    return lax.ppermute(x, "sec", [(i, i ^ 1) for i in range(count) if i ^ 1 < count])


def pass_far(x):
    count = lax.axis_size("sec")
    pairs = [(s, s + 2 if s % 2 == 0 else s - 2) for s in range(count)]
    pairs = [(s, t) for s, t in pairs if 0 <= t < count]
    sources = sorted(set(range(count)) - {s for s, _ in pairs})
    targets = sorted(set(range(count)) - {t for _, t in pairs})
    return lax.ppermute(x, "sec", pairs + list(zip(sources, targets)))


def far_exists():
    sector = lax.axis_index("sec")
    far = sector + 1 - 2 * lax.rem(sector + 1, 2)
    return (far >= 0) & (far < lax.axis_size("sec"))


def place(offset):
    near = 2 * lax.rem(lax.axis_index("sec"), 2) - 1
    return jnp.where(offset == 0, OWN, jnp.where(offset == near, NEAR, FAR))


def list_channels(shifts, order, wanted, start=0):
    count = jnp.int32(start)
    for channel in range(shifts.shape[0]):
        order[count] = channel
        count += jnp.where(place(shifts[channel]) == wanted, 1, 0)
    return count


def join(dst, mine, other, valid=None):
    parity = lax.rem(lax.axis_index("chan"), 2)
    half = mine.shape[0]
    dst[pl.ds(pl.multiple_of(parity * half, half), half), :] = mine[...]
    dst[pl.ds(pl.multiple_of((1 - parity) * half, half), half), :] = other[...]
    if valid is not None:

        @pl.when(jnp.logical_not(valid))
        def _():
            dst[...] = jnp.zeros_like(dst)


def by_twos(first, count, step):
    pairs = lax.div(count - first, 2)

    def body(i, carry):
        step(first + 2 * i, 2)
        return carry

    lax.fori_loop(0, pairs, body, 0)

    @pl.when(count - first > 2 * pairs)
    def _():
        step(count - 1, 1)


def add_terms(count, order, src, left, right, acc, ready):
    def step(i, n):
        channels = [order[i + j] for j in range(n)]
        for channel in channels:
            ready(channel)
        halfway = [
            jnp.dot(left[channel], src[...], preferred_element_type=F32).astype(BF16)
            for channel in channels
        ]
        terms = [
            lax.dot_general(h, right[channel], (((1,), (1,)), ((), ())), preferred_element_type=F32)
            for h, channel in zip(halfway, channels)
        ]
        acc[...] += sum(terms[1:], terms[0])

    by_twos(0, count, step)


def loader(left_in, right_in, left, right, order, left_sem, right_sem):
    def loads(channel):
        return (
            pltpu.make_async_copy(left_in.at[channel, 0], left.at[channel], left_sem.at[channel]),
            pltpu.make_async_copy(right_in.at[channel, 0], right.at[channel], right_sem.at[channel]),
        )

    def fetch(first, count):
        def body(i, carry):
            for copy in loads(order[i]):
                copy.start()
            return carry

        lax.fori_loop(first, count, body, 0)

    def ready(channel):
        for copy in loads(channel):
            copy.wait()

    def rest(first, count):
        def body(i, carry):
            ready(order[i])
            return carry

        lax.fori_loop(first, count, body, 0)

    return fetch, ready, rest


def own_sum_kernel(
    shifts_in, widths_in, state_in, left_in, right_in, acc, left, right, shifts,
    src, widths, order, small_sem, left_sem, right_sem
):
    small = [
        pltpu.make_async_copy(shifts_in, shifts, small_sem.at[0]),
        pltpu.make_async_copy(widths_in, widths, small_sem.at[1]),
        pltpu.make_async_copy(state_in.at[0], src, small_sem.at[2]),
    ]
    for copy in small:
        copy.start()
    fetch, ready, rest = loader(left_in, right_in, left, right, order, left_sem, right_sem)
    small[0].wait()
    owned = list_channels(shifts, order, OWN)
    near = list_channels(shifts, order, NEAR, owned)
    fetch(0, near)
    acc[...] = jnp.zeros_like(acc)
    small[1].wait()
    small[2].wait()
    rows = lax.broadcasted_iota(jnp.int32, src.shape, 0)
    cols = lax.broadcasted_iota(jnp.int32, src.shape, 1)
    inside = (rows < widths[0]) & (cols < widths[0])
    src[...] = jnp.where(inside, src[...], jnp.zeros_like(src))
    add_terms(owned, order, src, left, right, acc, ready)
    rest(owned, near)


def near_sum_kernel(
    shifts, mine, other, acc_in, left_old, right_old, left_in, right_in, acc, left, right,
    src, order, ahead, left_sem, right_sem
):
    far = list_channels(shifts, ahead, FAR)
    fetch, _, rest = loader(left_in, right_in, left, right, ahead, left_sem, right_sem)
    fetch(0, far)
    count = list_channels(shifts, order, NEAR)
    join(src, mine, other)
    acc[...] = acc_in[...]
    add_terms(count, order, src, left, right, acc, lambda channel: None)
    rest(0, far)


def far_sum_kernel(shifts, mine, other, acc_in, left, right, keep, give, acc, src, order):
    count = list_channels(shifts, order, FAR)
    join(src, mine, other, far_exists())
    acc[...] = acc_in[...]
    add_terms(count, order, src, left, right, acc, lambda channel: None)
    half = keep.shape[0]
    parity = lax.rem(lax.axis_index("chan"), 2)
    keep[...] = acc[pl.ds(pl.multiple_of(parity * half, half), half), :]
    give[...] = acc[pl.ds(pl.multiple_of((1 - parity) * half, half), half), :].astype(BF16)


def cost(matmuls, pad):
    return pl.CostEstimate(
        flops=int(matmuls * 2 * pad**3), transcendentals=0, bytes_accessed=int(matmuls * 2 * pad**2)
    )


def own_sum(shifts, widths, state, left, right):
    chans, _, pad, _ = left.shape
    blocks = jax.ShapeDtypeStruct((chans, pad, pad), BF16)
    return pl.pallas_call(
        own_sum_kernel,
        in_specs=[ANY] * 5,
        out_specs=[VMEM] * 3 + [SMEM],
        out_shape=[
            jax.ShapeDtypeStruct((pad, pad), F32),
            blocks,
            blocks,
            jax.ShapeDtypeStruct(shifts.shape, jnp.int32),
        ],
        scratch_shapes=[
            pltpu.VMEM((pad, pad), BF16),
            pltpu.SMEM(widths.shape, jnp.int32),
            pltpu.SMEM((chans + 1,), jnp.int32),
            pltpu.SemaphoreType.DMA((3,)),
            pltpu.SemaphoreType.DMA((chans,)),
            pltpu.SemaphoreType.DMA((chans,)),
        ],
        compiler_params=pltpu.CompilerParams(vmem_limit_bytes=ROOM),
        cost_estimate=cost(2 * chans / 3, pad),
        name="own_sum",
    )(in_hbm(shifts), widths, *[in_hbm(x) for x in (state, left, right)])


def near_sum(shifts, mine, other, acc, left, right, left_in, right_in):
    chans, pad, _ = left.shape
    blocks = jax.ShapeDtypeStruct((chans, pad, pad), BF16)
    return pl.pallas_call(
        near_sum_kernel,
        in_specs=[SMEM] + [VMEM] * 5 + [ANY] * 2,
        out_specs=[VMEM] * 3,
        out_shape=[jax.ShapeDtypeStruct((pad, pad), F32), blocks, blocks],
        scratch_shapes=[
            pltpu.VMEM((pad, pad), BF16),
            pltpu.SMEM((chans + 1,), jnp.int32),
            pltpu.SMEM((chans + 1,), jnp.int32),
            pltpu.SemaphoreType.DMA((chans,)),
            pltpu.SemaphoreType.DMA((chans,)),
        ],
        input_output_aliases={4: 1, 5: 2},
        compiler_params=pltpu.CompilerParams(vmem_limit_bytes=ROOM),
        cost_estimate=cost(2 * chans / 3, pad),
        name="near_sum",
    )(
        shifts,
        *[held(x) for x in (mine, other, acc, left, right)],
        *[in_hbm(x) for x in (left_in, right_in)],
    )


def far_sum(shifts, mine, other, acc, left, right):
    chans, pad, _ = left.shape
    half = pad // 2
    return pl.pallas_call(
        far_sum_kernel,
        in_specs=[SMEM] + [VMEM] * 5,
        out_specs=[VMEM] * 2,
        out_shape=[
            jax.ShapeDtypeStruct((half, pad), F32),
            jax.ShapeDtypeStruct((half, pad), BF16),
        ],
        scratch_shapes=[
            pltpu.VMEM((pad, pad), F32),
            pltpu.VMEM((pad, pad), BF16),
            pltpu.SMEM((chans + 1,), jnp.int32),
        ],
        compiler_params=pltpu.CompilerParams(vmem_limit_bytes=ROOM),
        cost_estimate=cost(2 * chans / 3, pad),
        name="far_sum",
    )(shifts, *[held(x) for x in (mine, other, acc, left, right)])


def finish(first, count, order, turned, src, new_left, obuf, osem, ready=None):
    scale = src.shape[0] ** (-0.5)

    def store(i):
        return pltpu.make_async_copy(obuf.at[i], new_left.at[order[i], 0], osem.at[i])

    def step(i, n):
        slots = [i + j for j in range(n)]
        bra_left = [ready[k] if turned is None else turned(order[k]) for k in slots]
        rotated = [jnp.dot(x, src[...], preferred_element_type=F32) for x in bra_left]
        for k, x in zip(slots, rotated):
            obuf[k] = (x * scale).astype(BF16)
            store(k).start()

    by_twos(first, count, step)

    def drain(i, carry):
        store(i).wait()
        return carry

    return lambda: lax.fori_loop(first, count, drain, 0)


def turn(bra, left, channel):
    return jnp.dot(bra[...], left[channel], preferred_element_type=F32).astype(BF16)


def turn_ahead(shifts, order, wanted, bra, left, half_turned):
    count = list_channels(shifts, order, wanted)

    def step(i, n):
        for k, x in [(i + j, turn(bra, left, order[i + j])) for j in range(n)]:
            half_turned[k] = x

    by_twos(0, count, step)


def own_turn_kernel(
    shifts, mine, other, left, rows, new_left, half_turned, bra, src, order, ahead, obuf, osem
):
    owned = list_channels(shifts, order, OWN)
    join(src, mine, other)
    bra[...] = src[...].T
    share = rows.shape[0]
    rows[...] = src[pl.ds(pl.multiple_of(lax.axis_index("chan") * share, share), share), :]
    drain = finish(
        0, owned, order, lambda channel: turn(bra, left, channel), src, new_left, obuf, osem
    )
    turn_ahead(shifts, ahead, NEAR, bra, left, half_turned)
    drain()


def turn_scratch(chans, pad):
    return [
        pltpu.VMEM((pad, pad), BF16),
        pltpu.SMEM((chans + 1,), jnp.int32),
        pltpu.SMEM((chans + 1,), jnp.int32),
        pltpu.VMEM((chans, pad, pad), BF16),
        pltpu.SemaphoreType.DMA((chans,)),
    ]


def own_turn(shifts, mine, other, left, share):
    chans, pad, _ = left.shape
    return pl.pallas_call(
        own_turn_kernel,
        in_specs=[SMEM, VMEM, VMEM, VMEM],
        out_specs=[VMEM, ANY, VMEM, VMEM],
        out_shape=[
            jax.ShapeDtypeStruct((share, pad), BF16),
            jax.ShapeDtypeStruct((chans, 1, pad, pad), BF16),
            jax.ShapeDtypeStruct((chans, pad, pad), BF16),
            jax.ShapeDtypeStruct((pad, pad), BF16),
        ],
        scratch_shapes=turn_scratch(chans, pad),
        compiler_params=pltpu.CompilerParams(vmem_limit_bytes=ROOM),
        cost_estimate=cost(chans, pad),
        name="own_turn",
    )(shifts, held(mine), held(other), held(left))


def near_turn_kernel(
    shifts, mine, other, half_turned, bra, left, old, new_left, far_turned, src, order, ahead, obuf, osem
):
    count = list_channels(shifts, order, NEAR)
    join(src, mine, other)
    drain = finish(0, count, order, None, src, new_left, obuf, osem, half_turned)
    turn_ahead(shifts, ahead, FAR, bra, left, far_turned)
    drain()


def near_turn(shifts, mine, other, half_turned, bra, left, new_left):
    chans, pad, _ = left.shape
    return pl.pallas_call(
        near_turn_kernel,
        in_specs=[SMEM] + [VMEM] * 5 + [ANY],
        out_specs=[ANY, VMEM],
        out_shape=[
            jax.ShapeDtypeStruct(new_left.shape, BF16),
            jax.ShapeDtypeStruct((chans, pad, pad), BF16),
        ],
        scratch_shapes=turn_scratch(chans, pad),
        input_output_aliases={6: 0},
        compiler_params=pltpu.CompilerParams(vmem_limit_bytes=ROOM),
        cost_estimate=cost(2 * chans / 3, pad),
        name="near_turn",
    )(shifts, *[held(x) for x in (mine, other, half_turned, bra, left)], new_left)


def far_turn_kernel(shifts, mine, other, far_turned, old, new_left, src, order, ahead, obuf, osem):
    count = list_channels(shifts, order, FAR)
    join(src, mine, other, far_exists())
    finish(0, count, order, None, src, new_left, obuf, osem, far_turned)()


def far_turn(shifts, mine, other, far_turned, new_left):
    chans, pad, _ = far_turned.shape
    return pl.pallas_call(
        far_turn_kernel,
        in_specs=[SMEM] + [VMEM] * 3 + [ANY],
        out_specs=ANY,
        out_shape=jax.ShapeDtypeStruct(new_left.shape, BF16),
        scratch_shapes=turn_scratch(chans, pad),
        input_output_aliases={4: 0},
        compiler_params=pltpu.CompilerParams(vmem_limit_bytes=ROOM),
        cost_estimate=cost(chans / 3, pad),
        name="far_turn",
    )(shifts, held(mine), held(other), held(far_turned), new_left)


def exchange(mine, chunks):
    rows = mine.shape[0] // chunks
    near, far = [], []
    for i in range(chunks):
        near.append(swap_near(mine[i * rows : (i + 1) * rows]))
    for i in range(chunks):
        far.append(pass_far(near[i]))
    near = held(jnp.concatenate(near))
    far = held(jnp.concatenate(far))
    near_other = swap_core(near)
    far_other = swap_core(far)
    return near, near_other, far, far_other


def body(state_blocks, left_blocks, right_blocks, widths, step_sizes, shifts):
    pad = state_blocks.shape[1]
    half = pad // 2
    chan_count = lax.axis_size("chan")
    first = lax.axis_index("chan") % 2 * half
    width = widths[0]
    positions = jnp.arange(pad, dtype=jnp.int32)
    inside = ((first + positions[:half]) < width)[:, None] & (positions < width)[None, :]
    state_m = lax.dynamic_slice_in_dim(state_blocks[0], first, half, 0)
    state_m = jnp.where(inside, state_m, jnp.zeros_like(state_m))

    near_m, near_o, far_m, far_o = exchange(state_m, 2)
    acc, left, right, shifts = own_sum(shifts, widths, state_blocks, left_blocks, right_blocks)
    acc, left, right = near_sum(shifts, near_m, near_o, acc, left, right, left_blocks, right_blocks)
    keep, give = far_sum(shifts, far_m, far_o, acc, left, right)

    pair_sum = (keep + swap_core(give).astype(F32)).astype(BF16)
    total = pair_sum.astype(F32)
    for turn in range(2, chan_count, 2):
        moved = lax.ppermute(
            pair_sum, "chan", [(i, (i + turn) % chan_count) for i in range(chan_count)]
        )
        total = total + moved.astype(F32)
    product = jnp.where(inside, total, jnp.zeros_like(total))
    corrected = state_m.astype(F32) - step_sizes[0] * product
    update_m = jnp.where(inside, corrected, jnp.zeros_like(corrected)).astype(BF16)

    near_m, near_o, far_m, far_o = exchange(update_m, 1)
    update_o = swap_core(update_m)
    rows, new_left, half_turned, bra = own_turn(shifts, update_m, update_o, left, pad // chan_count)
    new_left, far_turned = near_turn(
        shifts, near_m, near_o, half_turned, bra, left, new_left
    )
    new_left = far_turn(shifts, far_m, far_o, far_turned, new_left)
    return rows[None], new_left


def solution(mesh):
    placed = (
        P("sec", None, None),
        P("chan", "sec", None, None),
        P("chan", "sec", None, None),
        P("sec"),
        P("sec"),
        P("chan"),
    )
    return jax.shard_map(
        body,
        mesh=mesh,
        in_specs=placed,
        out_specs=(P("sec", "chan", None), P("chan", "sec", None, None)),
        check_vma=False,
    )
```
